32 devices in a mesh: sample: 2 (over x), sy: 4 (over y, core), sz: 4 (over z).
Axes of the slice: x: 2, y: 2, z: 4, core: 2. Of those that a mesh axis runs over, the one named last changes fastest.
Arguments:
- volume: bfloat16 [2, 32, 16, 32, 128], P('sample', None, 'sz', 'sy'), may hold values from -22.5 to 22.5
- amax_history: float32 [4, 16], replicated, may hold values from 0.48 to 2.5
- conv_first: bfloat16 [27, 32, 32], replicated, may hold values from -0.21875 to 0.21875
- conv_second: bfloat16 [27, 32, 32], replicated, may hold values from -0.21875 to 0.21875
- conv_third: bfloat16 [27, 64, 32], P(None, 'sy'), may hold values from -0.21875 to 0.21875
- conv_fourth: bfloat16 [27, 64, 64], P(None, 'sy'), may hold values from -0.15625 to 0.15625
- gain_fine: float32 [2, 32], replicated, may hold values from 0.5 to 1.5
- shift_fine: float32 [2, 32], replicated, may hold values from -0.5 to 0.5
- gain_coarse: float32 [2, 64], P(None, 'sy'), may hold values from 0.5 to 1.5
- shift_coarse: float32 [2, 64], P(None, 'sy'), may hold values from -0.5 to 0.5
Outputs:
- skip_features: bfloat16 [2, 32, 16, 32, 128], P('sample', None, 'sz', 'sy')
- coarse_features: bfloat16 [2, 64, 8, 1024], P('sample', 'sy', 'sz')
- amax_now: float32 [4], replicated
The draws below stay inside these ranges and needn't reach their ends.
All inputs are finite; a program needn't handle non-finite values.
Results may differ from the reference program's by a relative error of at most 0.012.
Values may be sent and summed in bfloat16 or wider, within the bound.
A program may use at most 128 MiB of HBM per device.

```python
import jax
import jax.numpy as jnp
from jax import lax

C1 = 32
C2 = 64
NX = 128
HIST = 16
LAYERS = 4
SAMPLES = 2
NY = 32
NZ = 16


def draw_volume(key, part):
    shape_all = (SAMPLES, C1, NZ, NY, NX)
    sample_pos = lax.broadcasted_iota(jnp.float32, shape_all, 0) / max(SAMPLES - 1, 1)
    z_pos = lax.broadcasted_iota(jnp.float32, shape_all, 2) / NZ
    y_pos = lax.broadcasted_iota(jnp.float32, shape_all, 3) / NY
    scaling = (0.6 + 1.2 * sample_pos) * (0.5 + z_pos + y_pos)
    noise_part = jnp.clip(jax.random.normal(key, shape_all, jnp.float32), -5.0, 5.0)
    return (noise_part * scaling).astype(jnp.bfloat16)


def draw_amax_history(key, part):
    level_key = jax.random.fold_in(key, 11)
    entry_key = jax.random.fold_in(key, 12)
    level_log = jax.random.uniform(level_key, (LAYERS, 1), jnp.float32, jnp.log(0.8), jnp.log(2.5))
    entries = jax.random.uniform(entry_key, (LAYERS, HIST), jnp.float32, 0.6, 1.0)
    return jnp.exp(level_log) * entries


def level_of(stream_key, dims, cuts, least, largest):
    def one(position, shards_of):
        steps = jax.random.uniform(jax.random.fold_in(jax.random.fold_in(stream_key, 6), position), (shards_of,), jnp.float32, least / len(cuts), largest / len(cuts))
        return jnp.repeat(jnp.exp(steps), dims[position] // shards_of).reshape((-1,) + (1,) * (len(dims) - position - 1))

    factor_of = one(*cuts[0])
    for cut in cuts[1:]:
        factor_of = factor_of * one(*cut)
    return factor_of


def gaussian(own_key, shape, scale, most, cuts=(), held_as=jnp.bfloat16):
    values = scale * jax.random.normal(own_key, shape, jnp.float32)
    if cuts:
        values = values * level_of(own_key, shape, cuts, -0.22, 0.18)
    return jnp.clip(values, -most, most).astype(held_as)


def setup_inputs(seed: int = 0) -> dict:
    seeds = jax.random.split(jax.random.key(seed), 11)
    volume = draw_volume(jax.random.fold_in(seeds[10], 71), 0)
    amax_history = draw_amax_history(jax.random.fold_in(seeds[10], 71), 0)
    conv_first = gaussian(seeds[2], (27, C1, C1), (27 * C1) ** -0.5, 0.21875)
    conv_second = gaussian(seeds[3], (27, C1, C1), (27 * C1) ** -0.5, 0.21875)
    conv_third = gaussian(seeds[4], (27, C2, C1), (27 * C1) ** -0.5, 0.21875, ((1, 4),))
    conv_fourth = gaussian(seeds[5], (27, C2, C2), (27 * C2) ** -0.5, 0.15625, ((1, 4),))
    gain_fine = jnp.clip(1.0 + 0.1 * jax.random.normal(seeds[6], (2, C1), jnp.float32), 0.5, 1.5)
    shift_fine = jnp.clip(jax.random.uniform(seeds[7], (2, C1), jnp.float32, -0.5, 0.5), -0.5, 0.5)
    gain_coarse = jnp.clip(1.0 + 0.1 * jax.random.normal(seeds[8], (2, C2), jnp.float32), 0.5, 1.5)
    shift_coarse = jnp.clip(jax.random.uniform(seeds[9], (2, C2), jnp.float32, -0.5, 0.5) * level_of(seeds[9], (2, C2), ((1, 4),), -0.4, 0.0), -0.5, 0.5)
    return {"volume": volume, "amax_history": amax_history, "conv_first": conv_first, "conv_second": conv_second, "conv_third": conv_third, "conv_fourth": conv_fourth, "gain_fine": gain_fine, "shift_fine": shift_fine, "gain_coarse": gain_coarse, "shift_coarse": shift_coarse}


norm_eps = 1e-05
leak_slope = 0.01

def convolve(values, weight):
    out_chan = weight.shape[1]
    in_chan = weight.shape[2]
    kernel = jnp.transpose(weight.reshape(3, 3, 3, out_chan, in_chan), (3, 4, 0, 1, 2))
    result = lax.conv_general_dilated(values.astype(jnp.float32)[None], kernel.astype(jnp.float32), (1, 1, 1), 'SAME', dimension_numbers=('NCDHW', 'OIDHW', 'NCDHW'), precision=lax.Precision.HIGHEST)
    return result[0]

def activate(values, gains, offset):
    cell_count = values[0].size
    flat_rows = values.reshape(values.shape[0], -1)
    chan_mean = lax.optimization_barrier(jnp.sum(flat_rows, axis=1)) / cell_count
    spread = lax.optimization_barrier(jnp.sum(flat_rows * flat_rows, axis=1)) / cell_count - chan_mean * chan_mean
    scaling = lax.rsqrt(spread + norm_eps) * gains
    normed = (values - chan_mean[:, None, None, None]) * scaling[:, None, None, None] + offset[:, None, None, None]
    return jnp.where(normed >= 0, normed, leak_slope * normed).astype(jnp.bfloat16)

def limited(values, bound):
    return jnp.clip(values.astype(jnp.float32), -bound, bound).astype(jnp.bfloat16)

def pool_max(values):
    chans, depth_cells, height_cells, width_cells = values.shape
    blocks = values.reshape(chans, depth_cells // 2, 2, height_cells // 2, 2, width_cells // 2, 2)
    return lax.optimization_barrier(jnp.max(blocks, axis=(2, 4, 6)))

def reference(volume, amax_history, conv_first, conv_second, conv_third, conv_fourth, gain_fine, shift_fine, gain_coarse, shift_coarse):
    bounds = lax.optimization_barrier(jnp.max(amax_history, axis=1))

    def single(volume_one):
        first = activate(convolve(limited(volume_one, bounds[0]), conv_first), gain_fine[0], shift_fine[0])
        skip_out = activate(convolve(limited(first, bounds[1]), conv_second), gain_fine[1], shift_fine[1])
        pooled = pool_max(skip_out)
        coarse = activate(convolve(limited(pooled, bounds[2]), conv_third), gain_coarse[0], shift_coarse[0])
        coarse_out = activate(convolve(limited(coarse, bounds[3]), conv_fourth), gain_coarse[1], shift_coarse[1])
        peak_list = jnp.stack([jnp.max(jnp.abs(member.astype(jnp.float32))) for member in (volume_one, first, pooled, coarse)])
        return (skip_out, coarse_out.reshape(coarse_out.shape[0], coarse_out.shape[1], -1), peak_list)
    skip_all, coarse_all, peak_all = lax.map(single, volume)
    return (skip_all, coarse_all, lax.optimization_barrier(jnp.max(peak_all, axis=0)))
```

```python
import functools

import jax
import jax.numpy as jnp
from jax import lax
from jax.experimental import pallas as pl
from jax.experimental.pallas import tpu as pltpu
from jax.sharding import PartitionSpec as P

norm_eps = 1e-05
leak_slope = 0.01
LANES = 128
MESH = pl.DeviceIdType.MESH
F32 = jnp.float32
BF16 = jnp.bfloat16
STEPS = ((-1, 0), (1, 0), (0, -1), (0, 1), (-1, -1), (-1, 1), (1, -1), (1, 1))


def iota(shape, dim):
    return lax.broadcasted_iota(jnp.int32, shape, dim)


def lane_row(column, start):
    n = column.shape[0]
    here = iota((n, LANES), 1) == iota((n, LANES), 0) + start
    return jnp.sum(jnp.where(here, column, 0.0), axis=0, keepdims=True)


def to_column(row, n, start):
    shape = (n, row.shape[1])
    here = iota(shape, 1) == iota(shape, 0) + start
    return jnp.sum(jnp.where(here, row, 0.0), axis=1, keepdims=True)


def leaky(normed):
    return jnp.where(normed >= 0, normed, leak_slope * normed).astype(BF16)


def remote(src, dst, send, recv, where):
    return pltpu.make_async_remote_copy(
        src_ref=src, dst_ref=dst, send_sem=send, recv_sem=recv, device_id=where, device_id_type=MESH
    )


def network(
    sizes,
    vol, hist, w1, w2, w3, w4, gf, sf, gc, sc,
    skip_out, coarse_out, peak_out,
    stacked, prod, vals, hid, zface, yface, corner,
    pool, wide3, g3, prod3, vals3, hid3, wide4, g4,
    stat, peak, peak_all,
    halo_s, halo_r, stat_s, stat_r, co_s, co_r, pk_s, pk_r, pa_s, pa_r,
):
    ns, ny, nz = sizes
    zc, yc, ch, xc = vol.shape
    hz, pairs = zc // 2, yc // 4
    tiles = pairs * ny
    oc = w3.shape[0] // 3
    group = ny * nz
    my_s, my_y, my_z = lax.axis_index("sample"), lax.axis_index("sy"), lax.axis_index("sz")
    me = my_y * nz + my_z

    def member(index):
        return {"sy": index // nz, "sz": lax.rem(index, nz)}

    barrier = pltpu.get_barrier_semaphore()
    for k in range(1, group):
        pl.semaphore_signal(barrier, inc=1, device_id=member(lax.rem(me + k, group)), device_id_type=MESH)
    for k in range(1, ns):
        pl.semaphore_signal(
            barrier, inc=1, device_id={"sample": lax.rem(my_s + k, ns)}, device_id_type=MESH
        )
    pl.semaphore_wait(barrier, group - 1 + ns - 1)

    lane = iota((ch, LANES), 1)
    bounds = [jnp.max(hist[l : l + 1, :]) for l in range(4)]

    def inside(dz, dy):
        z, y = my_z + dz, my_y + dy
        return (z >= 0) & (z < nz) & (y >= 0) & (y < ny)

    def halo(src, layer, d):
        dz, dy = STEPS[d]
        zi = 0 if dz < 0 else zc - 1
        yi = 0 if dy < 0 else yc - 1
        if dy == 0:
            src, dst = src.at[zi], zface.at[layer, int(dz < 0)]
        elif dz == 0:
            src, dst = src.at[:, yi], yface.at[layer, int(dy < 0)]
        else:
            src, dst = src.at[zi, yi], corner.at[layer, int(dz < 0) * 2 + int(dy < 0)]
        where = {"sy": jnp.clip(my_y + dy, 0, ny - 1), "sz": jnp.clip(my_z + dz, 0, nz - 1)}
        return remote(src, dst, halo_s.at[layer, d], halo_r.at[layer, d], where), dst

    def halo_start(src, layer):
        for d, (dz, dy) in enumerate(STEPS):
            @pl.when(inside(dz, dy))
            def _():
                halo(src, layer, d)[0].start()

            @pl.when(jnp.logical_not(inside(-dz, -dy)))
            def _():
                dst = halo(src, layer, d)[1]
                dst[...] = jnp.zeros(dst.shape, dst.dtype)

    def halo_wait(src, layer):
        for d, (dz, dy) in enumerate(STEPS):
            @pl.when(inside(-dz, -dy))
            def _():
                halo(src, layer, d)[0].wait_recv()

            @pl.when(inside(dz, dy))
            def _():
                halo(src, layer, d)[0].wait_send()

    def put(zp, yp, values, bound):
        v = jnp.clip(values.astype(F32), -bound, bound)
        left = jnp.where(lane == 0, 0.0, pltpu.roll(v, 1, 1))
        right = jnp.where(lane == LANES - 1, 0.0, pltpu.roll(v, LANES - 1, 1))
        stacked[zp, yp] = jnp.concatenate([left, v, right], axis=0).astype(BF16)

    def put_inner(src, bound):
        def plane(z, top):
            for y in range(yc):
                v = src[z, y]
                top = jnp.maximum(top, jnp.abs(v.astype(F32)))
                put(z + 1, y + 1, v, bound)
            return top

        return jnp.max(lax.fori_loop(0, zc, plane, jnp.zeros((ch, LANES), F32)))

    def put_halo(layer, bound):
        for side in range(2):
            for y in range(yc):
                put(side * (zc + 1), y + 1, zface[layer, side, y], bound)
            for z in range(zc):
                put(z + 1, side * (yc + 1), yface[layer, side, z], bound)
            for other in range(2):
                put(side * (zc + 1), other * (yc + 1), corner[layer, side * 2 + other], bound)

    def fine_conv(w):
        def plane(zp, carry):
            for y in range(0, yc, 2):
                rows = [stacked[zp, y + i : y + i + 3].reshape(9 * ch, LANES) for i in range(2)]
                prod[zp, y // 2] = jnp.dot(
                    w[...], jnp.concatenate(rows, axis=1), preferred_element_type=F32
                )
            return carry

        lax.fori_loop(0, zc + 2, plane, 0)

        def total(z, carry):
            s, q = carry
            for y in range(yc // 2):
                v = (
                    prod[z, y, 0:ch, :]
                    + prod[z + 1, y, ch : 2 * ch, :]
                    + prod[z + 2, y, 2 * ch : 3 * ch, :]
                )
                for i in range(2):
                    part = v[:, i * LANES : (i + 1) * LANES]
                    vals[z, 2 * y + i] = part
                    s, q = s + part, q + part * part
            return s, q

        zero = jnp.zeros((ch, LANES), F32)
        return lax.fori_loop(0, zc, total, (zero, zero))

    def share(buf, row, index, count, send, recv, where):
        buf[index] = jnp.broadcast_to(row, (8, LANES))

        def copy(k, slot):
            other = lax.rem(index + k, count)
            at = index if slot == "mine" else other
            return remote(buf.at[at], buf.at[at], send.at[k], recv.at[at], where(other))

        for k in range(1, count):
            copy(k, "mine").start()
        return copy

    def shared(copy, count):
        for k in range(1, count):
            copy(k, "theirs").wait_recv()
            copy(k, "mine").wait_send()

    def moments(phase, s, q, index, count, where, cells, gain_row, shift_row):
        n = s.shape[0]
        row = lane_row(jnp.sum(s, axis=1, keepdims=True), 0) + lane_row(
            jnp.sum(q, axis=1, keepdims=True), LANES // 2
        )
        buf = stat.at[phase]
        shared(share(buf, row, index, count, stat_s.at[phase], stat_r.at[phase], where), count)
        total = buf[0, 0:1, :]
        for i in range(1, count):
            total = total + buf[i, 0:1, :]
        mean = to_column(total, n, 0) / cells
        spread = to_column(total, n, LANES // 2) / cells - mean * mean
        scaling = lax.rsqrt(spread + norm_eps) * to_column(gain_row, n, 0)
        return mean, scaling, to_column(shift_row, n, 0)

    def fine_act(dst, phase, s, q):
        cells = float(zc * nz * yc * ny * xc)
        mean, scaling, offset = moments(
            phase, s, q, me, group, member, cells, gf[phase : phase + 1, :], sf[phase : phase + 1, :]
        )
        mean, scaling, offset = (jnp.broadcast_to(a, (ch, LANES)) for a in (mean, scaling, offset))

        def plane(z, carry):
            for y in range(yc):
                dst[z, y] = leaky((vals[z, y] - mean) * scaling + offset)
            return carry

        lax.fori_loop(0, zc, plane, 0)

    halo_start(vol, 0)
    peak0 = put_inner(vol, bounds[0])
    halo_wait(vol, 0)
    put_halo(0, bounds[0])
    s, q = fine_conv(w1)
    fine_act(hid, 0, s, q)
    halo_start(hid, 1)
    peak1 = put_inner(hid, bounds[1])
    halo_wait(hid, 1)
    put_halo(1, bounds[1])
    s, q = fine_conv(w2)
    fine_act(skip_out, 1, s, q)

    src_lane, dst_lane = iota((LANES, LANES), 0), iota((LANES, LANES), 1)
    half = LANES // 2
    pick = [
        jnp.where((dst_lane // half == i) & (src_lane == 2 * (dst_lane - i * half)), 1.0, 0.0).astype(BF16)
        for i in range(2)
    ]
    top = jnp.zeros((ch, LANES), F32)
    for z in range(hz):
        for t in range(pairs):
            found = jnp.zeros((ch, LANES), F32)
            for i in range(2):
                y = 4 * t + 2 * i
                block = [skip_out[2 * z + a, y + b].astype(F32) for a in range(2) for b in range(2)]
                m = jnp.maximum(jnp.maximum(block[0], block[1]), jnp.maximum(block[2], block[3]))
                m = jnp.maximum(m, pltpu.roll(m, LANES - 1, 1))
                found = found + jnp.dot(m.astype(BF16), pick[i], preferred_element_type=F32)
            top = jnp.maximum(top, jnp.abs(found))
            cells = jnp.clip(found, -bounds[2], bounds[2]).astype(BF16)
            pool[z, t] = cells
            g3[z + 1, my_y * pairs + t] = cells
    peak2 = jnp.max(top)

    def coarse_copies(layer, src, block_of, slab_of):
        out = []
        send, recv = co_s.at[layer], co_r.at[layer]
        for k in range(1, ny):
            other = lax.rem(my_y + k, ny)
            out.append((
                None,
                remote(src, slab_of(my_y), send.at[0, k], recv.at[0, my_y], {"sy": other}),
                None,
                remote(src, slab_of(other), send.at[0, k], recv.at[0, other], {"sy": other}),
            ))
        for kind, (step, plane, to) in enumerate(((-1, 0, hz + 1), (1, hz - 1, 0)), start=1):
            z = jnp.clip(my_z + step, 0, nz - 1)
            sends = (my_z + step >= 0) & (my_z + step < nz)
            gets = (my_z - step >= 0) & (my_z - step < nz)
            for y in range(ny):
                where = {"sy": y, "sz": z}
                out.append((
                    sends,
                    remote(src.at[plane], block_of(to, my_y), send.at[kind, y], recv.at[kind, my_y], where),
                    gets,
                    remote(src.at[plane], block_of(to, y), send.at[kind, y], recv.at[kind, y], where),
                ))
        return out

    def guarded(flag, act):
        if flag is None:
            act()
        else:
            pl.when(flag)(act)

    def coarse_start(copies, buf):
        for sends, mine, _, _ in copies:
            guarded(sends, mine.start)
        for at, missing in ((0, my_z == 0), (hz + 1, my_z == nz - 1)):
            @pl.when(missing)
            def _():
                buf[at] = jnp.zeros(buf.shape[1:], buf.dtype)

    def coarse_wait(copies):
        for sends, mine, gets, theirs in copies:
            guarded(gets, theirs.wait_recv)
            guarded(sends, mine.wait_send)

    def widen(load, n, wide):
        where = iota((n, LANES), 1)
        column = lax.rem(where, half)
        low = iota((3 * n, LANES), 1) < half

        def plane(z, carry):
            def put3(k, t, v):
                wide[z, k * 3 * n : (k + 1) * 3 * n, t * LANES : (t + 1) * LANES] = v.astype(BF16)

            before = jnp.zeros((3 * n, LANES), F32)
            for t in range(tiles):
                v = load(z, t).astype(F32)
                left = jnp.where(column == 0, 0.0, pltpu.roll(v, 1, 1))
                right = jnp.where(column == half - 1, 0.0, pltpu.roll(v, LANES - 1, 1))
                x = jnp.concatenate([left, v, right], axis=0)
                u = pltpu.roll(x, half, 1)
                put3(1, t, x)
                put3(0, t, jnp.where(low, before, u))
                if t:
                    put3(2, t - 1, jnp.where(low, before, u))
                before = u
            put3(2, tiles - 1, jnp.where(low, before, 0.0))
            return carry

        lax.fori_loop(0, hz + 2, plane, 0)

    def coarse_conv(w, wide):
        def plane(z, carry):
            prod3[z] = jnp.dot(w[...], wide[z], preferred_element_type=F32)
            return carry

        lax.fori_loop(0, hz + 2, plane, 0)
        s = q = jnp.zeros((oc, LANES), F32)
        for z in range(hz):
            for t in range(tiles):
                cols = slice(t * LANES, (t + 1) * LANES)
                v = (
                    prod3[z, 0:oc, cols]
                    + prod3[z + 1, oc : 2 * oc, cols]
                    + prod3[z + 2, 2 * oc : 3 * oc, cols]
                )
                vals3[z, :, cols] = v
                s, q = s + v, q + v * v
        return s, q

    coarse_cells = float(hz * nz * tiles * LANES)

    def slab(index):
        return {"sz": index}

    copies = coarse_copies(
        0,
        pool,
        lambda plane, y: g3.at[plane, pl.ds(y * pairs, pairs)],
        lambda y: g3.at[pl.ds(1, hz), pl.ds(y * pairs, pairs)],
    )
    coarse_start(copies, g3)
    coarse_wait(copies)
    widen(lambda z, t: g3[z, t], ch, wide3)
    s, q = coarse_conv(w3, wide3)
    mean, scaling, offset = moments(2, s, q, my_z, nz, slab, coarse_cells, gc[0:1, :], sc[0:1, :])
    top = jnp.zeros((oc, tiles * LANES), F32)
    for z in range(hz):
        v = leaky((vals3[z] - mean) * scaling + offset).astype(F32)
        top = jnp.maximum(top, jnp.abs(v))
        v = jnp.clip(v, -bounds[3], bounds[3]).astype(BF16)
        hid3[z] = v
        g4[z + 1, my_y] = v
    peak3 = jnp.max(top)
    copies = coarse_copies(
        1, hid3, lambda plane, y: g4.at[plane, y], lambda y: g4.at[pl.ds(1, hz), y]
    )
    coarse_start(copies, g4)

    at = iota((1, LANES), 1)
    row = jnp.zeros((1, LANES), F32)
    for i, value in enumerate((peak0, peak1, peak2, peak3)):
        row = jnp.where(at == i, value, row)
    peaks = share(peak, row, me, group, pk_s, pk_r, member)
    coarse_wait(copies)
    widen(
        lambda z, t: g4[z, :, :, t * LANES : (t + 1) * LANES].reshape(ny * oc, LANES), ny * oc, wide4
    )
    shared(peaks, group)
    row = peak[0, 0:1, :]
    for i in range(1, group):
        row = jnp.maximum(row, peak[i, 0:1, :])
    peaks = share(peak_all, row, my_s, ns, pa_s, pa_r, lambda index: {"sample": index})
    s, q = coarse_conv(w4, wide4)
    mean, scaling, offset = moments(3, s, q, my_z, nz, slab, coarse_cells, gc[1:2, :], sc[1:2, :])
    for z in range(hz):
        coarse_out[z] = leaky((vals3[z] - mean) * scaling + offset)
    shared(peaks, ns)
    row = peak_all[0]
    for i in range(1, ns):
        row = jnp.maximum(row, peak_all[i])
    peak_out[...] = row


def per_device(sizes, volume, hist, c1, c2, c3, c4, gf, sf, gc, sc):
    ns, ny, nz = sizes
    _, ch, zc, yc, xc = volume.shape
    oc = c3.shape[1]
    hz, pairs = zc // 2, yc // 4
    tiles = pairs * ny
    flat = tiles * LANES
    assert xc == LANES and zc % 2 == 0 and yc % 4 == 0

    def matrix(w):
        taps, out, inner = w.shape
        w = w.reshape(3, 9, out, inner)
        return jnp.transpose(w, (0, 2, 1, 3)).reshape(3 * out, 9 * inner)

    vmem = pl.BlockSpec(memory_space=pltpu.VMEM)
    dma = pltpu.SemaphoreType.DMA
    group = ny * nz
    skip, coarse, peaks = pl.pallas_call(
        functools.partial(network, sizes),
        out_shape=(
            jax.ShapeDtypeStruct((zc, yc, ch, xc), BF16),
            jax.ShapeDtypeStruct((hz, oc, flat), BF16),
            jax.ShapeDtypeStruct((8, LANES), F32),
        ),
        in_specs=[vmem] * 10,
        out_specs=(vmem,) * 3,
        scratch_shapes=[
            pltpu.VMEM((zc + 2, yc + 2, 3 * ch, LANES), BF16),
            pltpu.VMEM((zc + 2, yc // 2, 3 * ch, 2 * LANES), F32),
            pltpu.VMEM((zc, yc, ch, LANES), F32),
            pltpu.VMEM((zc, yc, ch, LANES), BF16),
            pltpu.VMEM((2, 2, yc, ch, LANES), BF16),
            pltpu.VMEM((2, 2, zc, ch, LANES), BF16),
            pltpu.VMEM((2, 4, ch, LANES), BF16),
            pltpu.VMEM((hz, pairs, ch, LANES), BF16),
            pltpu.VMEM((hz + 2, 9 * ch, flat), BF16),
            pltpu.VMEM((hz + 2, tiles, ch, LANES), BF16),
            pltpu.VMEM((hz + 2, 3 * oc, flat), F32),
            pltpu.VMEM((hz, oc, flat), F32),
            pltpu.VMEM((hz, oc, flat), BF16),
            pltpu.VMEM((hz + 2, 9 * oc * ny, flat), BF16),
            pltpu.VMEM((hz + 2, ny, oc, flat), BF16),
            pltpu.VMEM((4, group, 8, LANES), F32),
            pltpu.VMEM((group, 8, LANES), F32),
            pltpu.VMEM((ns, 8, LANES), F32),
            dma((2, 8)),
            dma((2, 8)),
            dma((4, group)),
            dma((4, group)),
            dma((2, 3, ny)),
            dma((2, 3, ny)),
            dma((group,)),
            dma((group,)),
            dma((ns,)),
            dma((ns,)),
        ],
        compiler_params=pltpu.CompilerParams(
            collective_id=0, has_side_effects=True, vmem_limit_bytes=56 * 1024 * 1024
        ),
    )(
        jnp.transpose(volume[0], (1, 2, 0, 3)),
        hist, matrix(c1), matrix(c2), matrix(c3), matrix(c4), gf, sf, gc, sc,
    )
    return (
        jnp.transpose(skip, (2, 0, 1, 3))[None],
        jnp.transpose(coarse, (1, 0, 2))[None],
        peaks[0, :4],
    )


def solution(mesh):
    sizes = (mesh.shape["sample"], mesh.shape["sy"], mesh.shape["sz"])
    return jax.shard_map(
        functools.partial(per_device, sizes),
        mesh=mesh,
        in_specs=(
            P("sample", None, "sz", "sy", None),
            P(),
            P(),
            P(),
            P(None, "sy", None),
            P(None, "sy", None),
            P(),
            P(),
            P(None, "sy"),
            P(None, "sy"),
        ),
        out_specs=(P("sample", None, "sz", "sy", None), P("sample", "sy", "sz", None), P()),
        check_vma=False,
    )
```

```python
import functools

import jax
import jax.numpy as jnp
from jax import lax
from jax.experimental import pallas as pl
from jax.experimental.pallas import tpu as pltpu
from jax.sharding import PartitionSpec as P

norm_eps = 1e-05
leak_slope = 0.01
LANES = 128
MESH = pl.DeviceIdType.MESH
F32 = jnp.float32
BF16 = jnp.bfloat16
STEPS = ((-1, 0), (1, 0), (0, -1), (0, 1), (-1, -1), (-1, 1), (1, -1), (1, 1))


def iota(shape, dim):
    return lax.broadcasted_iota(jnp.int32, shape, dim)


def lane_row(column, start):
    n = column.shape[0]
    here = iota((n, LANES), 1) == iota((n, LANES), 0) + start
    return jnp.sum(jnp.where(here, column, 0.0), axis=0, keepdims=True)


def to_column(row, n, start):
    shape = (n, row.shape[1])
    here = iota(shape, 1) == iota(shape, 0) + start
    return jnp.sum(jnp.where(here, row, 0.0), axis=1, keepdims=True)


def leaky(normed):
    return jnp.where(normed >= 0, normed, leak_slope * normed).astype(BF16)


def remote(src, dst, send, recv, where):
    return pltpu.make_async_remote_copy(
        src_ref=src, dst_ref=dst, send_sem=send, recv_sem=recv, device_id=where, device_id_type=MESH
    )


def network(
    sizes,
    volume, hist, c1, c2, c3, c4, gf, sf, gc, sc,
    skip_out, coarse_out, peak_out,
    w1, w2, w3, w4, turn, vol, skip,
    stacked, prod, vals, hid, zface, yface, corner,
    pool, wide3, g3, prod3, vals3, hid3, wide4, g4,
    stat, peak, peak_all,
    halo_s, halo_r, stat_s, stat_r, co_s, co_r, pk_s, pk_r, pa_s, pa_r,
):
    ns, ny, nz = sizes
    zc, yc, ch, xc = vol.shape
    hz, pairs = zc // 2, yc // 4
    tiles = pairs * ny
    oc = c3.shape[1]
    group = ny * nz
    my_s, my_y, my_z = lax.axis_index("sample"), lax.axis_index("sy"), lax.axis_index("sz")
    me = my_y * nz + my_z

    def member(index):
        return {"sy": index // nz, "sz": lax.rem(index, nz)}

    barrier = pltpu.get_barrier_semaphore()
    for k in range(1, group):
        pl.semaphore_signal(barrier, inc=1, device_id=member(lax.rem(me + k, group)), device_id_type=MESH)
    for k in range(1, ns):
        pl.semaphore_signal(
            barrier, inc=1, device_id={"sample": lax.rem(my_s + k, ns)}, device_id_type=MESH
        )

    for matrix, taps in ((w1, c1), (w2, c2), (w3, c3), (w4, c4)):
        out = taps.shape[1]
        for a in range(3):
            parts = [taps[9 * a + k].astype(F32) for k in range(9)]
            matrix[a * out : (a + 1) * out, :] = jnp.concatenate(parts, axis=1).astype(BF16)
    for z in range(zc):
        turn[z] = volume[:, z].astype(F32).reshape(ch * yc, LANES)
    for z in range(zc):
        for y in range(yc):
            vol[z, y] = turn[z, pl.ds(y, ch, yc), :].astype(BF16)
    pl.semaphore_wait(barrier, group - 1 + ns - 1)

    lane = iota((ch, LANES), 1)
    bounds = [jnp.max(hist[l : l + 1, :]) for l in range(4)]

    def inside(dz, dy):
        z, y = my_z + dz, my_y + dy
        return (z >= 0) & (z < nz) & (y >= 0) & (y < ny)

    def landing(layer, d):
        dz, dy = STEPS[d]
        if dy == 0:
            return zface.at[layer, int(dz < 0)]
        if dz == 0:
            return yface.at[layer, int(dy < 0)]
        return corner.at[layer, int(dz < 0) * 2 + int(dy < 0)]

    def halo(src, layer, d):
        dz, dy = STEPS[d]
        zi = 0 if dz < 0 else zc - 1
        yi = 0 if dy < 0 else yc - 1
        if dy == 0:
            src = src.at[zi]
        elif dz == 0:
            src = src.at[:, yi]
        else:
            src = src.at[zi, yi]
        where = {"sy": jnp.clip(my_y + dy, 0, ny - 1), "sz": jnp.clip(my_z + dz, 0, nz - 1)}
        return remote(src, landing(layer, d), halo_s.at[layer, d], halo_r.at[layer, d], where)

    def halo_start(src, layer):
        for d, (dz, dy) in enumerate(STEPS):
            @pl.when(inside(dz, dy))
            def _():
                halo(src, layer, d).start()

            @pl.when(jnp.logical_not(inside(-dz, -dy)))
            def _():
                dst = landing(layer, d)
                dst[...] = jnp.zeros(dst.shape, dst.dtype)

    def halo_wait(src, layer, flat):
        for d, (dz, dy) in enumerate(STEPS):
            if (dz == 0) != flat:
                continue

            @pl.when(inside(-dz, -dy))
            def _():
                halo(src, layer, d).wait_recv()

            @pl.when(inside(dz, dy))
            def _():
                halo(src, layer, d).wait_send()

    def put(zp, yp, values, bound):
        v = jnp.clip(values.astype(F32), -bound, bound)
        left = jnp.where(lane == 0, 0.0, pltpu.roll(v, 1, 1))
        right = jnp.where(lane == LANES - 1, 0.0, pltpu.roll(v, LANES - 1, 1))
        stacked[zp, yp] = jnp.concatenate([left, v, right], axis=0).astype(BF16)

    def put_inner(src, bound):
        def plane(z, top):
            for y in range(yc):
                v = src[z, y]
                top = jnp.maximum(top, jnp.abs(v.astype(F32)))
                put(z + 1, y + 1, v, bound)
            return top

        return jnp.max(lax.fori_loop(0, zc, plane, jnp.zeros((ch, LANES), F32)))

    def put_sides(layer, bound):
        for side in range(2):
            for z in range(zc):
                put(z + 1, side * (yc + 1), yface[layer, side, z], bound)

    def put_ends(layer, bound):
        for side in range(2):
            for y in range(yc):
                put(side * (zc + 1), y + 1, zface[layer, side, y], bound)
            for other in range(2):
                put(side * (zc + 1), other * (yc + 1), corner[layer, side * 2 + other], bound)

    def fine_conv(w, src, layer, bound):
        def plane(zp, carry):
            for y in range(0, yc, 2):
                rows = [stacked[zp, y + i : y + i + 3].reshape(9 * ch, LANES) for i in range(2)]
                prod[zp, y // 2] = jnp.dot(
                    w[...], jnp.concatenate(rows, axis=1), preferred_element_type=F32
                )
            return carry

        halo_wait(src, layer, True)
        put_sides(layer, bound)
        lax.fori_loop(1, zc + 1, plane, 0)
        halo_wait(src, layer, False)
        put_ends(layer, bound)
        lax.fori_loop(0, 2, lambda i, carry: plane(i * (zc + 1), carry), 0)

        def total(z, carry):
            s, q = carry
            for y in range(yc // 2):
                v = (
                    prod[z, y, 0:ch, :]
                    + prod[z + 1, y, ch : 2 * ch, :]
                    + prod[z + 2, y, 2 * ch : 3 * ch, :]
                )
                for i in range(2):
                    part = v[:, i * LANES : (i + 1) * LANES]
                    vals[z, 2 * y + i] = part
                    s, q = s + part, q + part * part
            return s, q

        zero = jnp.zeros((ch, LANES), F32)
        return lax.fori_loop(0, zc, total, (zero, zero))

    def share(buf, row, index, count, send, recv, where):
        buf[index, 0:1, :] = row

        def copy(k, slot):
            other = lax.rem(index + k, count)
            at = index if slot == "mine" else other
            ref = buf.at[at, pl.ds(0, 1)]
            return remote(ref, ref, send.at[k], recv.at[at], where(other))

        for k in range(1, count):
            copy(k, "mine").start()
        return copy

    def shared(copy, count):
        for k in range(1, count):
            copy(k, "theirs").wait_recv()
            copy(k, "mine").wait_send()

    def moments(phase, s, q, index, count, where, cells, gain_row, shift_row):
        n = s.shape[0]
        row = lane_row(jnp.sum(s, axis=1, keepdims=True), 0) + lane_row(
            jnp.sum(q, axis=1, keepdims=True), LANES // 2
        )
        buf = stat.at[phase]
        shared(share(buf, row, index, count, stat_s.at[phase], stat_r.at[phase], where), count)
        total = buf[0, 0:1, :]
        for i in range(1, count):
            total = total + buf[i, 0:1, :]
        mean = to_column(total, n, 0) / cells
        spread = to_column(total, n, LANES // 2) / cells - mean * mean
        scaling = lax.rsqrt(spread + norm_eps) * to_column(gain_row, n, 0)
        return mean, scaling, to_column(shift_row, n, 0)

    def fine_act(dst, phase, s, q):
        cells = float(zc * nz * yc * ny * xc)
        mean, scaling, offset = moments(
            phase, s, q, me, group, member, cells, gf[phase : phase + 1, :], sf[phase : phase + 1, :]
        )
        mean, scaling, offset = (jnp.broadcast_to(a, (ch, LANES)) for a in (mean, scaling, offset))

        def plane(z, carry):
            for y in range(yc):
                dst[z, y] = leaky((vals[z, y] - mean) * scaling + offset)
            return carry

        lax.fori_loop(0, zc, plane, 0)

    halo_start(vol, 0)
    peak0 = put_inner(vol, bounds[0])
    s, q = fine_conv(w1, vol, 0, bounds[0])
    fine_act(hid, 0, s, q)
    halo_start(hid, 1)
    peak1 = put_inner(hid, bounds[1])
    s, q = fine_conv(w2, hid, 1, bounds[1])
    fine_act(skip, 1, s, q)

    src_lane, dst_lane = iota((LANES, LANES), 0), iota((LANES, LANES), 1)
    half = LANES // 2
    pick = [
        jnp.where((dst_lane // half == i) & (src_lane == 2 * (dst_lane - i * half)), 1.0, 0.0).astype(BF16)
        for i in range(2)
    ]
    top = jnp.zeros((ch, LANES), F32)
    for z in range(hz):
        for t in range(pairs):
            found = jnp.zeros((ch, LANES), F32)
            for i in range(2):
                y = 4 * t + 2 * i
                block = [skip[2 * z + a, y + b].astype(F32) for a in range(2) for b in range(2)]
                m = jnp.maximum(jnp.maximum(block[0], block[1]), jnp.maximum(block[2], block[3]))
                m = jnp.maximum(m, pltpu.roll(m, LANES - 1, 1))
                found = found + jnp.dot(m.astype(BF16), pick[i], preferred_element_type=F32)
            top = jnp.maximum(top, jnp.abs(found))
            cells = jnp.clip(found, -bounds[2], bounds[2]).astype(BF16)
            pool[z, t] = cells
            g3[z + 1, my_y * pairs + t] = cells
    peak2 = jnp.max(top)

    def coarse_copies(layer, src, block_of, slab_of):
        out = []
        send, recv = co_s.at[layer], co_r.at[layer]
        for k in range(1, ny):
            other = lax.rem(my_y + k, ny)
            out.append((
                True,
                remote(src, slab_of(my_y), send.at[0, k], recv.at[0, my_y], {"sy": other}),
                True,
                remote(src, slab_of(other), send.at[0, k], recv.at[0, other], {"sy": other}),
            ))
        for kind, (step, plane, to) in enumerate(((-1, 0, hz + 1), (1, hz - 1, 0)), start=1):
            z = jnp.clip(my_z + step, 0, nz - 1)
            sends = (my_z + step >= 0) & (my_z + step < nz)
            gets = (my_z - step >= 0) & (my_z - step < nz)
            for y in range(ny):
                where = {"sy": y, "sz": z}
                out.append((
                    sends,
                    remote(src.at[plane], block_of(to, my_y), send.at[kind, y], recv.at[kind, my_y], where),
                    gets,
                    remote(src.at[plane], block_of(to, y), send.at[kind, y], recv.at[kind, y], where),
                ))
        return out

    def guarded(flag, act):
        if flag is True:
            act()
        else:
            pl.when(flag)(act)

    def coarse_start(copies, buf):
        for sends, mine, _, _ in copies:
            guarded(sends, mine.start)
        for at, missing in ((0, my_z == 0), (hz + 1, my_z == nz - 1)):
            @pl.when(missing)
            def _():
                buf[at] = jnp.zeros(buf.shape[1:], buf.dtype)

    def coarse_wait(copies, slab):
        for sends, mine, gets, theirs in copies:
            if (sends is True) != slab:
                continue
            guarded(gets, theirs.wait_recv)
            guarded(sends, mine.wait_send)

    def widen(load, n, wide):
        where = iota((n, LANES), 1)
        column = lax.rem(where, half)
        low = iota((3 * n, LANES), 1) < half

        def plane(z):
            def put3(k, t, v):
                wide[z, k * 3 * n : (k + 1) * 3 * n, t * LANES : (t + 1) * LANES] = v.astype(BF16)

            before = jnp.zeros((3 * n, LANES), F32)
            for t in range(tiles):
                v = load(z, t).astype(F32)
                left = jnp.where(column == 0, 0.0, pltpu.roll(v, 1, 1))
                right = jnp.where(column == half - 1, 0.0, pltpu.roll(v, LANES - 1, 1))
                x = jnp.concatenate([left, v, right], axis=0)
                u = pltpu.roll(x, half, 1)
                put3(1, t, x)
                put3(0, t, jnp.where(low, before, u))
                if t:
                    put3(2, t - 1, jnp.where(low, before, u))
                before = u
            put3(2, tiles - 1, jnp.where(low, before, 0.0))

        return plane

    def coarse_conv(w, wide, load, n, copies):
        widen_plane = widen(load, n, wide)

        def plane(z, carry):
            widen_plane(z)
            prod3[z] = jnp.dot(w[...], wide[z], preferred_element_type=F32)
            return carry

        coarse_wait(copies, True)
        lax.fori_loop(1, hz + 1, plane, 0)
        coarse_wait(copies, False)
        lax.fori_loop(0, 2, lambda i, carry: plane(i * (hz + 1), carry), 0)

    def coarse_sums():
        s = q = jnp.zeros((oc, LANES), F32)
        for z in range(hz):
            for t in range(tiles):
                cols = slice(t * LANES, (t + 1) * LANES)
                v = (
                    prod3[z, 0:oc, cols]
                    + prod3[z + 1, oc : 2 * oc, cols]
                    + prod3[z + 2, 2 * oc : 3 * oc, cols]
                )
                vals3[z, :, cols] = v
                s, q = s + v, q + v * v
        return s, q

    coarse_cells = float(hz * nz * tiles * LANES)

    def slab(index):
        return {"sz": index}

    copies = coarse_copies(
        0,
        pool,
        lambda plane, y: g3.at[plane, pl.ds(y * pairs, pairs)],
        lambda y: g3.at[pl.ds(1, hz), pl.ds(y * pairs, pairs)],
    )
    coarse_start(copies, g3)
    for z in range(zc):
        for y in range(yc):
            turn[z, pl.ds(y, ch, yc), :] = skip[z, y].astype(F32)
    for z in range(zc):
        skip_out[:, z] = turn[z].reshape(ch, yc, LANES).astype(BF16)
    coarse_conv(w3, wide3, lambda z, t: g3[z, t], ch, copies)
    s, q = coarse_sums()
    mean, scaling, offset = moments(2, s, q, my_z, nz, slab, coarse_cells, gc[0:1, :], sc[0:1, :])
    top = jnp.zeros((oc, tiles * LANES), F32)
    for z in range(hz):
        v = leaky((vals3[z] - mean) * scaling + offset).astype(F32)
        top = jnp.maximum(top, jnp.abs(v))
        v = jnp.clip(v, -bounds[3], bounds[3]).astype(BF16)
        hid3[z] = v
        g4[z + 1, my_y] = v
    peak3 = jnp.max(top)
    copies = coarse_copies(
        1, hid3, lambda plane, y: g4.at[plane, y], lambda y: g4.at[pl.ds(1, hz), y]
    )
    coarse_start(copies, g4)

    at = iota((1, LANES), 1)
    row = jnp.zeros((1, LANES), F32)
    for i, value in enumerate((peak0, peak1, peak2, peak3)):
        row = jnp.where(at == i, value, row)
    peaks = share(peak, row, me, group, pk_s, pk_r, member)

    def cells4(z, t):
        return g4[z, :, :, t * LANES : (t + 1) * LANES].reshape(ny * oc, LANES)

    coarse_conv(w4, wide4, cells4, ny * oc, copies)
    shared(peaks, group)
    row = peak[0, 0:1, :]
    for i in range(1, group):
        row = jnp.maximum(row, peak[i, 0:1, :])
    peaks = share(peak_all, row, my_s, ns, pa_s, pa_r, lambda index: {"sample": index})
    s, q = coarse_sums()
    mean, scaling, offset = moments(3, s, q, my_z, nz, slab, coarse_cells, gc[1:2, :], sc[1:2, :])
    for z in range(hz):
        coarse_out[:, z, :] = leaky((vals3[z] - mean) * scaling + offset)
    shared(peaks, ns)
    row = peak_all[0, 0:1, :]
    for i in range(1, ns):
        row = jnp.maximum(row, peak_all[i, 0:1, :])
    for i in range(4):
        peak_out[i] = jnp.max(jnp.where(at == i, row, 0.0))


def per_device(sizes, volume, hist, c1, c2, c3, c4, gf, sf, gc, sc):
    ns, ny, nz = sizes
    _, ch, zc, yc, xc = volume.shape
    oc = c3.shape[1]
    hz, pairs = zc // 2, yc // 4
    tiles = pairs * ny
    flat = tiles * LANES
    assert xc == LANES and zc % 2 == 0 and yc % 4 == 0

    vmem = pl.BlockSpec(memory_space=pltpu.VMEM)
    dma = pltpu.SemaphoreType.DMA
    group = ny * nz
    skip, coarse, peaks = pl.pallas_call(
        functools.partial(network, sizes),
        out_shape=(
            jax.ShapeDtypeStruct((ch, zc, yc, xc), BF16),
            jax.ShapeDtypeStruct((oc, hz, flat), BF16),
            jax.ShapeDtypeStruct((4,), F32),
        ),
        in_specs=[vmem] * 10,
        out_specs=(vmem, vmem, pl.BlockSpec(memory_space=pltpu.SMEM)),
        scratch_shapes=[
            pltpu.VMEM((3 * ch, 9 * ch), BF16),
            pltpu.VMEM((3 * ch, 9 * ch), BF16),
            pltpu.VMEM((3 * oc, 9 * ch), BF16),
            pltpu.VMEM((3 * oc, 9 * oc * ny), BF16),
            pltpu.VMEM((zc, ch * yc, LANES), F32),
            pltpu.VMEM((zc, yc, ch, LANES), BF16),
            pltpu.VMEM((zc, yc, ch, LANES), BF16),
            pltpu.VMEM((zc + 2, yc + 2, 3 * ch, LANES), BF16),
            pltpu.VMEM((zc + 2, yc // 2, 3 * ch, 2 * LANES), F32),
            pltpu.VMEM((zc, yc, ch, LANES), F32),
            pltpu.VMEM((zc, yc, ch, LANES), BF16),
            pltpu.VMEM((2, 2, yc, ch, LANES), BF16),
            pltpu.VMEM((2, 2, zc, ch, LANES), BF16),
            pltpu.VMEM((2, 4, ch, LANES), BF16),
            pltpu.VMEM((hz, pairs, ch, LANES), BF16),
            pltpu.VMEM((hz + 2, 9 * ch, flat), BF16),
            pltpu.VMEM((hz + 2, tiles, ch, LANES), BF16),
            pltpu.VMEM((hz + 2, 3 * oc, flat), F32),
            pltpu.VMEM((hz, oc, flat), F32),
            pltpu.VMEM((hz, oc, flat), BF16),
            pltpu.VMEM((hz + 2, 9 * oc * ny, flat), BF16),
            pltpu.VMEM((hz + 2, ny, oc, flat), BF16),
            pltpu.VMEM((4, group, 8, LANES), F32),
            pltpu.VMEM((group, 8, LANES), F32),
            pltpu.VMEM((ns, 8, LANES), F32),
            dma((2, 8)),
            dma((2, 8)),
            dma((4, group)),
            dma((4, group)),
            dma((2, 3, ny)),
            dma((2, 3, ny)),
            dma((group,)),
            dma((group,)),
            dma((ns,)),
            dma((ns,)),
        ],
        compiler_params=pltpu.CompilerParams(
            collective_id=0, has_side_effects=True, vmem_limit_bytes=56 * 1024 * 1024
        ),
    )(volume[0], hist, c1, c2, c3, c4, gf, sf, gc, sc)
    return skip[None], coarse[None], peaks


def solution(mesh):
    sizes = (mesh.shape["sample"], mesh.shape["sy"], mesh.shape["sz"])
    return jax.shard_map(
        functools.partial(per_device, sizes),
        mesh=mesh,
        in_specs=(
            P("sample", None, "sz", "sy", None),
            P(),
            P(),
            P(),
            P(None, "sy", None),
            P(None, "sy", None),
            P(),
            P(),
            P(None, "sy"),
            P(None, "sy"),
        ),
        out_specs=(P("sample", None, "sz", "sy", None), P("sample", "sy", "sz", None), P()),
        check_vma=False,
    )
```

```python
import functools

import jax
import jax.numpy as jnp
from jax import lax
from jax.experimental import pallas as pl
from jax.experimental.pallas import tpu as pltpu
from jax.sharding import PartitionSpec as P

norm_eps = 1e-05
leak_slope = 0.01
LANES = 128
MESH = pl.DeviceIdType.MESH
F32 = jnp.float32
BF16 = jnp.bfloat16
STEPS = ((-1, 0), (1, 0), (0, -1), (0, 1), (-1, -1), (-1, 1), (1, -1), (1, 1))


def iota(shape, dim):
    return lax.broadcasted_iota(jnp.int32, shape, dim)


def lane_row(column, start):
    n = column.shape[0]
    here = iota((n, LANES), 1) == iota((n, LANES), 0) + start
    return jnp.sum(jnp.where(here, column, 0.0), axis=0, keepdims=True)


def to_column(row, n, start):
    shape = (n, row.shape[1])
    here = iota(shape, 1) == iota(shape, 0) + start
    return jnp.sum(jnp.where(here, row, 0.0), axis=1, keepdims=True)


def leaky(normed):
    return jnp.where(normed >= 0, normed, leak_slope * normed).astype(BF16)


def remote(src, dst, send, recv, where):
    return pltpu.make_async_remote_copy(
        src_ref=src, dst_ref=dst, send_sem=send, recv_sem=recv, device_id=where, device_id_type=MESH
    )


def network(
    sizes,
    volume, hist, c1, c2, c3, c4, gf, sf, gc, sc,
    skip_out, coarse_out, peak_out,
    w1, w2, w3, w4, turn, vol, skip,
    stacked, prod, vals, hid, zface, yface, corner,
    pool, wide3, g3, prod3, vals3, hid3, wide4, g4,
    stat, peak, peak_all,
    halo_s, halo_r, stat_s, stat_r, co_s, co_r, pk_s, pk_r, pa_s, pa_r,
):
    ns, ny, nz = sizes
    zc, yc, ch, xc = vol.shape
    hz, pairs = zc // 2, yc // 4
    tiles = pairs * ny
    oc = c3.shape[1]
    group = ny * nz
    my_s, my_y, my_z = lax.axis_index("sample"), lax.axis_index("sy"), lax.axis_index("sz")
    me = my_y * nz + my_z

    def member(index):
        return {"sy": index // nz, "sz": lax.rem(index, nz)}

    barrier = pltpu.get_barrier_semaphore()
    for k in range(1, group):
        pl.semaphore_signal(barrier, inc=1, device_id=member(lax.rem(me + k, group)), device_id_type=MESH)
    for k in range(1, ns):
        pl.semaphore_signal(
            barrier, inc=1, device_id={"sample": lax.rem(my_s + k, ns)}, device_id_type=MESH
        )

    for matrix, taps in ((w1, c1), (w2, c2), (w3, c3), (w4, c4)):
        out = taps.shape[1]
        for a in range(3):
            parts = [taps[9 * a + k].astype(F32) for k in range(9)]
            matrix[a * out : (a + 1) * out, :] = jnp.concatenate(parts, axis=1).astype(BF16)
    for z in range(zc):
        turn[z] = volume[:, z].astype(F32).reshape(ch * yc, LANES)
    for z in range(zc):
        for y in range(yc):
            vol[z, y] = turn[z, pl.ds(y, ch, yc), :].astype(BF16)
    pl.semaphore_wait(barrier, group - 1 + ns - 1)

    lane = iota((ch, LANES), 1)
    bounds = [jnp.max(hist[l : l + 1, :]) for l in range(4)]

    def inside(dz, dy):
        z, y = my_z + dz, my_y + dy
        return (z >= 0) & (z < nz) & (y >= 0) & (y < ny)

    def landing(layer, d):
        dz, dy = STEPS[d]
        if dy == 0:
            return zface.at[layer, int(dz < 0)]
        if dz == 0:
            return yface.at[layer, int(dy < 0)]
        return corner.at[layer, int(dz < 0) * 2 + int(dy < 0)]

    def halo(src, layer, d):
        dz, dy = STEPS[d]
        zi = 0 if dz < 0 else zc - 1
        yi = 0 if dy < 0 else yc - 1
        if dy == 0:
            src = src.at[zi]
        elif dz == 0:
            src = src.at[:, yi]
        else:
            src = src.at[zi, yi]
        where = {"sy": jnp.clip(my_y + dy, 0, ny - 1), "sz": jnp.clip(my_z + dz, 0, nz - 1)}
        return remote(src, landing(layer, d), halo_s.at[layer, d], halo_r.at[layer, d], where)

    def halo_start(src, layer):
        for d, (dz, dy) in enumerate(STEPS):
            @pl.when(inside(dz, dy))
            def _():
                halo(src, layer, d).start()

            @pl.when(jnp.logical_not(inside(-dz, -dy)))
            def _():
                dst = landing(layer, d)
                dst[...] = jnp.zeros(dst.shape, dst.dtype)

    def halo_wait(src, layer, flat):
        for d, (dz, dy) in enumerate(STEPS):
            if (dz == 0) != flat:
                continue

            @pl.when(inside(-dz, -dy))
            def _():
                halo(src, layer, d).wait_recv()

            @pl.when(inside(dz, dy))
            def _():
                halo(src, layer, d).wait_send()

    def put(zp, yp, values, bound):
        v = jnp.clip(values.astype(F32), -bound, bound)
        left = jnp.where(lane == 0, 0.0, pltpu.roll(v, 1, 1))
        right = jnp.where(lane == LANES - 1, 0.0, pltpu.roll(v, LANES - 1, 1))
        stacked[zp, yp] = jnp.concatenate([left, v, right], axis=0).astype(BF16)

    def put_inner(src, bound):
        def plane(z, top):
            for y in range(yc):
                v = src[z, y]
                top = jnp.maximum(top, jnp.abs(v.astype(F32)))
                put(z + 1, y + 1, v, bound)
            return top

        return jnp.max(lax.fori_loop(0, zc, plane, jnp.zeros((ch, LANES), F32)))

    def put_sides(layer, bound):
        for side in range(2):
            for z in range(zc):
                put(z + 1, side * (yc + 1), yface[layer, side, z], bound)

    def put_ends(layer, bound):
        for side in range(2):
            for y in range(yc):
                put(side * (zc + 1), y + 1, zface[layer, side, y], bound)
            for other in range(2):
                put(side * (zc + 1), other * (yc + 1), corner[layer, side * 2 + other], bound)

    def fine_conv(w, src, layer, bound):
        def plane(zp, carry):
            for y in range(0, yc, 2):
                rows = [stacked[zp, y + i : y + i + 3].reshape(9 * ch, LANES) for i in range(2)]
                prod[zp, y // 2] = jnp.dot(
                    w[...], jnp.concatenate(rows, axis=1), preferred_element_type=F32
                )
            return carry

        halo_wait(src, layer, True)
        put_sides(layer, bound)
        lax.fori_loop(1, zc + 1, plane, 0)
        halo_wait(src, layer, False)
        put_ends(layer, bound)
        lax.fori_loop(0, 2, lambda i, carry: plane(i * (zc + 1), carry), 0)

        def total(z, carry):
            s, q = carry
            for y in range(yc // 2):
                v = (
                    prod[z, y, 0:ch, :]
                    + prod[z + 1, y, ch : 2 * ch, :]
                    + prod[z + 2, y, 2 * ch : 3 * ch, :]
                )
                for i in range(2):
                    part = v[:, i * LANES : (i + 1) * LANES]
                    vals[z, 2 * y + i] = part
                    s, q = s + part, q + part * part
            return s, q

        zero = jnp.zeros((ch, LANES), F32)
        return lax.fori_loop(0, zc, total, (zero, zero))

    def share(buf, row, index, count, send, recv, where):
        buf[index, 0:1, :] = row

        def copy(k, slot):
            other = lax.rem(index + k, count)
            at = index if slot == "mine" else other
            ref = buf.at[at, pl.ds(0, 1)]
            return remote(ref, ref, send.at[k], recv.at[at], where(other))

        for k in sorted(range(1, count), key=lambda k: -min(k % nz, -k % nz)):
            copy(k, "mine").start()
        return copy

    def shared(copy, count):
        for k in range(1, count):
            copy(k, "theirs").wait_recv()
            copy(k, "mine").wait_send()

    def moments(phase, s, q, index, count, where, cells, gain_row, shift_row):
        n = s.shape[0]
        row = lane_row(jnp.sum(s, axis=1, keepdims=True), 0) + lane_row(
            jnp.sum(q, axis=1, keepdims=True), LANES // 2
        )
        buf = stat.at[phase]
        shared(share(buf, row, index, count, stat_s.at[phase], stat_r.at[phase], where), count)
        total = buf[0, 0:1, :]
        for i in range(1, count):
            total = total + buf[i, 0:1, :]
        mean = to_column(total, n, 0) / cells
        spread = to_column(total, n, LANES // 2) / cells - mean * mean
        scaling = lax.rsqrt(spread + norm_eps) * to_column(gain_row, n, 0)
        return mean, scaling, to_column(shift_row, n, 0)

    def fine_act(dst, phase, s, q):
        cells = float(zc * nz * yc * ny * xc)
        mean, scaling, offset = moments(
            phase, s, q, me, group, member, cells, gf[phase : phase + 1, :], sf[phase : phase + 1, :]
        )
        mean, scaling, offset = (jnp.broadcast_to(a, (ch, LANES)) for a in (mean, scaling, offset))

        def plane(z, carry):
            for y in range(yc):
                dst[z, y] = leaky((vals[z, y] - mean) * scaling + offset)
            return carry

        lax.fori_loop(0, zc, plane, 0)

    halo_start(vol, 0)
    peak0 = put_inner(vol, bounds[0])
    s, q = fine_conv(w1, vol, 0, bounds[0])
    fine_act(hid, 0, s, q)
    halo_start(hid, 1)
    peak1 = put_inner(hid, bounds[1])
    s, q = fine_conv(w2, hid, 1, bounds[1])
    fine_act(skip, 1, s, q)

    src_lane, dst_lane = iota((LANES, LANES), 0), iota((LANES, LANES), 1)
    half = LANES // 2
    pick = [
        jnp.where((dst_lane // half == i) & (src_lane == 2 * (dst_lane - i * half)), 1.0, 0.0).astype(BF16)
        for i in range(2)
    ]
    top = jnp.zeros((ch, LANES), F32)
    for z in range(hz):
        for t in range(pairs):
            found = jnp.zeros((ch, LANES), F32)
            for i in range(2):
                y = 4 * t + 2 * i
                block = [skip[2 * z + a, y + b].astype(F32) for a in range(2) for b in range(2)]
                m = jnp.maximum(jnp.maximum(block[0], block[1]), jnp.maximum(block[2], block[3]))
                m = jnp.maximum(m, pltpu.roll(m, LANES - 1, 1))
                found = found + jnp.dot(m.astype(BF16), pick[i], preferred_element_type=F32)
            top = jnp.maximum(top, jnp.abs(found))
            cells = jnp.clip(found, -bounds[2], bounds[2]).astype(BF16)
            pool[z, t] = cells
            g3[z + 1, my_y * pairs + t] = cells
    peak2 = jnp.max(top)

    def coarse_copies(layer, src, block_of, slab_of):
        out = []
        send, recv = co_s.at[layer], co_r.at[layer]
        for k in range(1, ny):
            other = lax.rem(my_y + k, ny)
            out.append((
                True,
                remote(src, slab_of(my_y), send.at[0, k], recv.at[0, my_y], {"sy": other}),
                True,
                remote(src, slab_of(other), send.at[0, k], recv.at[0, other], {"sy": other}),
            ))
        for kind, (step, plane, to) in enumerate(((-1, 0, hz + 1), (1, hz - 1, 0)), start=1):
            z = jnp.clip(my_z + step, 0, nz - 1)
            sends = (my_z + step >= 0) & (my_z + step < nz)
            gets = (my_z - step >= 0) & (my_z - step < nz)
            for y in range(ny):
                where = {"sy": y, "sz": z}
                out.append((
                    sends,
                    remote(src.at[plane], block_of(to, my_y), send.at[kind, y], recv.at[kind, my_y], where),
                    gets,
                    remote(src.at[plane], block_of(to, y), send.at[kind, y], recv.at[kind, y], where),
                ))
        return out

    def guarded(flag, act):
        if flag is True:
            act()
        else:
            pl.when(flag)(act)

    def coarse_start(copies, buf):
        for sends, mine, _, _ in copies:
            guarded(sends, mine.start)
        for at, missing in ((0, my_z == 0), (hz + 1, my_z == nz - 1)):
            @pl.when(missing)
            def _():
                buf[at] = jnp.zeros(buf.shape[1:], buf.dtype)

    def coarse_wait(copies, slab):
        for sends, mine, gets, theirs in copies:
            if (sends is True) != slab:
                continue
            guarded(gets, theirs.wait_recv)
            guarded(sends, mine.wait_send)

    def widen(load, n, wide):
        where = iota((n, LANES), 1)
        column = lax.rem(where, half)
        low = iota((3 * n, LANES), 1) < half

        def plane(z):
            def put3(k, t, v):
                wide[z, k * 3 * n : (k + 1) * 3 * n, t * LANES : (t + 1) * LANES] = v.astype(BF16)

            before = jnp.zeros((3 * n, LANES), F32)
            for t in range(tiles):
                v = load(z, t).astype(F32)
                left = jnp.where(column == 0, 0.0, pltpu.roll(v, 1, 1))
                right = jnp.where(column == half - 1, 0.0, pltpu.roll(v, LANES - 1, 1))
                x = jnp.concatenate([left, v, right], axis=0)
                u = pltpu.roll(x, half, 1)
                put3(1, t, x)
                put3(0, t, jnp.where(low, before, u))
                if t:
                    put3(2, t - 1, jnp.where(low, before, u))
                before = u
            put3(2, tiles - 1, jnp.where(low, before, 0.0))

        return plane

    def coarse_conv(w, wide, load, n, copies):
        widen_plane = widen(load, n, wide)

        def plane(z, carry):
            widen_plane(z)
            prod3[z] = jnp.dot(w[...], wide[z], preferred_element_type=F32)
            return carry

        coarse_wait(copies, True)
        lax.fori_loop(1, hz + 1, plane, 0)
        coarse_wait(copies, False)
        lax.fori_loop(0, 2, lambda i, carry: plane(i * (hz + 1), carry), 0)

    def coarse_sums():
        s = q = jnp.zeros((oc, LANES), F32)
        for z in range(hz):
            for t in range(tiles):
                cols = slice(t * LANES, (t + 1) * LANES)
                v = (
                    prod3[z, 0:oc, cols]
                    + prod3[z + 1, oc : 2 * oc, cols]
                    + prod3[z + 2, 2 * oc : 3 * oc, cols]
                )
                vals3[z, :, cols] = v
                s, q = s + v, q + v * v
        return s, q

    coarse_cells = float(hz * nz * tiles * LANES)

    def slab(index):
        return {"sz": index}

    copies = coarse_copies(
        0,
        pool,
        lambda plane, y: g3.at[plane, pl.ds(y * pairs, pairs)],
        lambda y: g3.at[pl.ds(1, hz), pl.ds(y * pairs, pairs)],
    )
    coarse_start(copies, g3)
    for z in range(zc):
        for y in range(yc):
            turn[z, pl.ds(y, ch, yc), :] = skip[z, y].astype(F32)
    for z in range(zc):
        skip_out[:, z] = turn[z].reshape(ch, yc, LANES).astype(BF16)
    coarse_conv(w3, wide3, lambda z, t: g3[z, t], ch, copies)
    s, q = coarse_sums()
    mean, scaling, offset = moments(2, s, q, my_z, nz, slab, coarse_cells, gc[0:1, :], sc[0:1, :])
    top = jnp.zeros((oc, tiles * LANES), F32)
    for z in range(hz):
        v = leaky((vals3[z] - mean) * scaling + offset).astype(F32)
        top = jnp.maximum(top, jnp.abs(v))
        v = jnp.clip(v, -bounds[3], bounds[3]).astype(BF16)
        hid3[z] = v
        g4[z + 1, my_y] = v
    peak3 = jnp.max(top)
    copies = coarse_copies(
        1, hid3, lambda plane, y: g4.at[plane, y], lambda y: g4.at[pl.ds(1, hz), y]
    )
    coarse_start(copies, g4)

    at = iota((1, LANES), 1)
    row = jnp.zeros((1, LANES), F32)
    for i, value in enumerate((peak0, peak1, peak2, peak3)):
        row = jnp.where(at == i, value, row)
    peaks = share(peak, row, me, group, pk_s, pk_r, member)

    def cells4(z, t):
        return g4[z, :, :, t * LANES : (t + 1) * LANES].reshape(ny * oc, LANES)

    coarse_conv(w4, wide4, cells4, ny * oc, copies)
    shared(peaks, group)
    row = peak[0, 0:1, :]
    for i in range(1, group):
        row = jnp.maximum(row, peak[i, 0:1, :])
    peaks = share(peak_all, row, my_s, ns, pa_s, pa_r, lambda index: {"sample": index})
    s, q = coarse_sums()
    mean, scaling, offset = moments(3, s, q, my_z, nz, slab, coarse_cells, gc[1:2, :], sc[1:2, :])
    for z in range(hz):
        coarse_out[:, z, :] = leaky((vals3[z] - mean) * scaling + offset)
    shared(peaks, ns)
    row = peak_all[0, 0:1, :]
    for i in range(1, ns):
        row = jnp.maximum(row, peak_all[i, 0:1, :])
    for i in range(4):
        peak_out[i] = jnp.max(jnp.where(at == i, row, 0.0))


def per_device(sizes, volume, hist, c1, c2, c3, c4, gf, sf, gc, sc):
    ns, ny, nz = sizes
    _, ch, zc, yc, xc = volume.shape
    oc = c3.shape[1]
    hz, pairs = zc // 2, yc // 4
    tiles = pairs * ny
    flat = tiles * LANES
    assert xc == LANES and zc % 2 == 0 and yc % 4 == 0

    vmem = pl.BlockSpec(memory_space=pltpu.VMEM)
    dma = pltpu.SemaphoreType.DMA
    group = ny * nz
    skip, coarse, peaks = pl.pallas_call(
        functools.partial(network, sizes),
        out_shape=(
            jax.ShapeDtypeStruct((ch, zc, yc, xc), BF16),
            jax.ShapeDtypeStruct((oc, hz, flat), BF16),
            jax.ShapeDtypeStruct((4,), F32),
        ),
        in_specs=[vmem] * 10,
        out_specs=(vmem, vmem, pl.BlockSpec(memory_space=pltpu.SMEM)),
        scratch_shapes=[
            pltpu.VMEM((3 * ch, 9 * ch), BF16),
            pltpu.VMEM((3 * ch, 9 * ch), BF16),
            pltpu.VMEM((3 * oc, 9 * ch), BF16),
            pltpu.VMEM((3 * oc, 9 * oc * ny), BF16),
            pltpu.VMEM((zc, ch * yc, LANES), F32),
            pltpu.VMEM((zc, yc, ch, LANES), BF16),
            pltpu.VMEM((zc, yc, ch, LANES), BF16),
            pltpu.VMEM((zc + 2, yc + 2, 3 * ch, LANES), BF16),
            pltpu.VMEM((zc + 2, yc // 2, 3 * ch, 2 * LANES), F32),
            pltpu.VMEM((zc, yc, ch, LANES), F32),
            pltpu.VMEM((zc, yc, ch, LANES), BF16),
            pltpu.VMEM((2, 2, yc, ch, LANES), BF16),
            pltpu.VMEM((2, 2, zc, ch, LANES), BF16),
            pltpu.VMEM((2, 4, ch, LANES), BF16),
            pltpu.VMEM((hz, pairs, ch, LANES), BF16),
            pltpu.VMEM((hz + 2, 9 * ch, flat), BF16),
            pltpu.VMEM((hz + 2, tiles, ch, LANES), BF16),
            pltpu.VMEM((hz + 2, 3 * oc, flat), F32),
            pltpu.VMEM((hz, oc, flat), F32),
            pltpu.VMEM((hz, oc, flat), BF16),
            pltpu.VMEM((hz + 2, 9 * oc * ny, flat), BF16),
            pltpu.VMEM((hz + 2, ny, oc, flat), BF16),
            pltpu.VMEM((4, group, 8, LANES), F32),
            pltpu.VMEM((group, 8, LANES), F32),
            pltpu.VMEM((ns, 8, LANES), F32),
            dma((2, 8)),
            dma((2, 8)),
            dma((4, group)),
            dma((4, group)),
            dma((2, 3, ny)),
            dma((2, 3, ny)),
            dma((group,)),
            dma((group,)),
            dma((ns,)),
            dma((ns,)),
        ],
        compiler_params=pltpu.CompilerParams(
            collective_id=0, has_side_effects=True, vmem_limit_bytes=56 * 1024 * 1024
        ),
    )(volume[0], hist, c1, c2, c3, c4, gf, sf, gc, sc)
    def finish(a, b, c, oa, ob, oc_):
        oa[...] = a[...]
        ob[...] = b[...]
        for i in range(4):
            oc_[i] = c[i]

    smem = pl.BlockSpec(memory_space=pltpu.SMEM)
    skip, coarse, peaks = pl.pallas_call(
        finish,
        out_shape=tuple(jax.ShapeDtypeStruct(a.shape, a.dtype) for a in (skip, coarse, peaks)),
        in_specs=[vmem, vmem, smem],
        out_specs=(vmem, vmem, smem),
    )(skip, coarse, peaks)
    return skip[None], coarse[None], peaks


def solution(mesh):
    sizes = (mesh.shape["sample"], mesh.shape["sy"], mesh.shape["sz"])
    return jax.shard_map(
        functools.partial(per_device, sizes),
        mesh=mesh,
        in_specs=(
            P("sample", None, "sz", "sy", None),
            P(),
            P(),
            P(),
            P(None, "sy", None),
            P(None, "sy", None),
            P(),
            P(),
            P(None, "sy"),
            P(None, "sy"),
        ),
        out_specs=(P("sample", None, "sz", "sy", None), P("sample", "sy", "sz", None), P()),
        check_vma=False,
    )
```
